32 devices in a mesh: row: 8 (over z, core), col: 2 (over y), head: 2 (over x).
Axes of the slice: x: 2, y: 2, z: 4, core: 2. Of those that a mesh axis runs over, the one named last changes fastest.
Arguments:
- x_lo: float32 [6, 32, 64, 4], P('col', 'row', 'head'), may hold values from -32 to 32
- noise: float32 [6, 32, 64, 16], P('col', 'row'), may hold values from -6 to 6
- t_index: int32 [6], P('col'), may hold values from 0 to 999
- labels: int32 [6], P('col'), may hold values from 0 to 1000
- stale_kv: bfloat16 [2, 6, 16, 32, 1152], P(None, 'col', 'row', None, 'head'), may hold values from -6 to 6
- embed_w: float32 [16, 1152], replicated, may hold values from -1.5 to 1.5
- t_w1: bfloat16 [256, 1152], replicated, may hold values from -0.375 to 0.375
- t_w2: bfloat16 [1152, 1152], P(None, 'row'), may hold values from -0.1875 to 0.1875
- class_table: bfloat16 [1001, 1152], P(None, 'row'), may hold values from -6 to 6
- ada_w: bfloat16 [1152, 6912], P('row'), may hold values from -0.1875 to 0.1875
- qkv_w: bfloat16 [1152, 3, 1152], P(None, None, 'head'), may hold values from -0.1875 to 0.1875
- out_w: bfloat16 [1152, 1152], P('head'), may hold values from -0.1875 to 0.1875
- fc1_w: bfloat16 [1152, 4608], P(None, ('col', 'head')), may hold values from -0.1875 to 0.1875
- fc2_w: bfloat16 [1152, 4608], P(None, ('col', 'head')), may hold values from -0.09375 to 0.09375
Outputs:
- tokens_out: bfloat16 [6, 32, 64, 1152], P('col', 'row', 'head')
The draws below stay inside these ranges and needn't reach their ends.
All inputs are finite; a program needn't handle non-finite values.
Results may differ from the reference program's by a relative error of at most 0.025.
Values may be sent and summed in bfloat16 or wider, within the bound.
No kernel may reach another device: no remote copies, remote signals or barrier semaphores. Data moves between devices by JAX's collectives and lax.ppermute only.
A program may use at most 128 MiB of HBM per device.

```python
import math
import jax
import jax.numpy as jnp
from jax import lax

HEADS = 16
HD = 72
D = 1152
FF = 4608
NCLASS = 1001
FREQ = 256
C = 4
TSTEPS = 1000
TR = 4
GC = 64
B = 6
GR = 32
LR = 16
LC = 32
N_ROW = 8


def draw_x_lo(key, part):
    subkeys = jax.random.split(key, 4)
    row_values = jnp.arange(GR, dtype=jnp.float32)
    row_scale = jnp.exp(math.log(3.0) * row_values / (GR - 1))
    rough = jnp.exp(jax.random.uniform(subkeys[0], (B, GR, GC, C), minval=math.log(0.5), maxval=math.log(2.0)))
    offset = jax.random.uniform(subkeys[1], (B, 1, 1, C), minval=-1.0, maxval=1.0)
    base_values = jnp.clip(jax.random.normal(subkeys[3], (B, GR, GC, C)), -4.0, 4.0)
    values = base_values * row_scale[None, :, None, None] * rough + offset
    return values.astype(jnp.float32)


def set_ends(values, own_key, least, largest):
    index_at = [jax.random.randint(jax.random.fold_in(own_key, axis), (), 0, length) for axis, length in enumerate(values.shape)]
    longest = values.shape.index(max(values.shape))
    neighbour = index_at[:longest] + [(index_at[longest] + 1) % values.shape[longest]] + index_at[longest + 1:]
    return values.at[tuple(index_at)].set(least).at[tuple(neighbour)].set(largest)


def levels(stream_key, shape, pieces, smallest, high):
    level = 1.0
    for axis_at, blocks in pieces:
        steps = jax.random.uniform(jax.random.fold_in(jax.random.fold_in(stream_key, 6), axis_at), (blocks,), jnp.float32, smallest / len(pieces), high / len(pieces))
        level = level * jnp.repeat(jnp.exp(steps), shape[axis_at] // blocks).reshape((-1,) + (1,) * (len(shape) - 1 - axis_at))
    return level


def gaussian(stream_key, shape, deviation, limit, cuts=(), kind=jnp.bfloat16):
    values = jax.random.normal(stream_key, shape, jnp.float32) * deviation
    if len(cuts) > 0:
        values = levels(stream_key, shape, cuts, -0.22, 0.18) * values
    return jnp.clip(values, min=-limit, max=limit).astype(kind)


def setup_inputs(seed: int = 0) -> dict:
    seeds = jax.random.split(jax.random.key(seed), 15)
    x_lo = draw_x_lo(jax.random.fold_in(seeds[14], 71), 0)
    noise = gaussian(seeds[1], (B, GR, GC, 4 * C), 1.0, 6.0, ((0, 2), (1, 8)), jnp.float32)
    t_index = set_ends(jax.random.randint(seeds[2], (B,), 0, TSTEPS), jax.random.fold_in(seeds[2], 1), 0, TSTEPS - 1).astype(jnp.int32)
    labels = set_ends(jax.random.randint(seeds[3], (B,), 0, NCLASS), jax.random.fold_in(seeds[3], 1), 0, NCLASS - 1).astype(jnp.int32)
    stale_kv = gaussian(seeds[4], (2, B, LR, LC, D), 1.0, 6.0, ((1, 2), (2, 8), (4, 2)))
    embed_w = gaussian(seeds[5], (4 * C, D), (4 * C) ** -0.5, 1.5, (), jnp.float32)
    t_w1 = gaussian(seeds[6], (FREQ, D), FREQ ** -0.5, 0.375)
    t_w2 = gaussian(seeds[7], (D, D), D ** -0.5, 0.1875, ((1, 8),))
    class_table = gaussian(seeds[8], (NCLASS, D), 1.0, 6.0, ((1, 8),))
    ada_w = gaussian(seeds[9], (D, 6 * D), D ** -0.5, 0.1875, ((0, 8),))
    qkv_w = gaussian(seeds[10], (D, 3, D), D ** -0.5, 0.1875, ((2, 2),))
    out_w = gaussian(seeds[11], (D, D), D ** -0.5, 0.1875, ((0, 2),))
    fc1_w = gaussian(seeds[12], (D, FF), D ** -0.5, 0.1875, ((1, 4),))
    fc2_w = gaussian(seeds[13], (D, FF), FF ** -0.5, 0.09375, ((1, 4),))
    return dict(x_lo=x_lo, noise=noise, t_index=t_index, labels=labels, stale_kv=stale_kv, embed_w=embed_w, t_w1=t_w1, t_w2=t_w2, class_table=class_table, ada_w=ada_w, qkv_w=qkv_w, out_w=out_w, fc1_w=fc1_w, fc2_w=fc2_w)


def upsample_padded(padded):
    upper = padded[:, :-2]
    middle = padded[:, 1:-1]
    lower = padded[:, 2:]
    rows_even = 0.75 * middle + 0.25 * upper
    rows_odd = 0.75 * middle + 0.25 * lower

    def widen(vertical):
        left_side = vertical[:, :, :-2]
        centre = vertical[:, :, 1:-1]
        right_side = vertical[:, :, 2:]
        return jnp.stack([0.75 * centre + 0.25 * left_side, 0.75 * centre + 0.25 * right_side], axis=3)
    stacked = jnp.stack([widen(rows_even), widen(rows_odd)], axis=3)
    return stacked.reshape(stacked.shape[0], stacked.shape[1], stacked.shape[2], 4 * stacked.shape[-1])

def noise_level(t_index):
    step_values = jnp.arange(TSTEPS, dtype=jnp.float32)
    betas = 0.0001 + (0.02 - 0.0001) * step_values / (TSTEPS - 1)
    log_keep = jnp.cumsum(jnp.log(1.0 - betas))
    picked = (jnp.arange(TSTEPS, dtype=jnp.int32)[None, :] == t_index[:, None]).astype(jnp.float32)
    return jnp.exp(lax.optimization_barrier(jnp.sum(picked * log_keep[None, :], axis=1)))

def position_table(row_pos, col_pos, width):
    quarter = width // 4
    omega = 1.0 / 10000.0 ** (jnp.arange(quarter, dtype=jnp.float32) / quarter)
    row_args = row_pos[:, None] * omega[None, :]
    col_args = col_pos[:, None] * omega[None, :]
    row_part = jnp.concatenate([jnp.sin(row_args), jnp.cos(row_args)], axis=1)
    col_part = jnp.concatenate([jnp.sin(col_args), jnp.cos(col_args)], axis=1)
    n_rows = row_pos.shape[0]
    n_cols = col_pos.shape[0]
    return jnp.concatenate([jnp.broadcast_to(row_part[:, None, :], (n_rows, n_cols, width // 2)), jnp.broadcast_to(col_part[None, :, :], (n_rows, n_cols, width // 2))], axis=2)

def condition(t_index, labels, t_w1, t_w2, class_table):
    half_freq = t_w1.shape[0] // 2
    freqs = jnp.exp(-math.log(10000.0) * jnp.arange(half_freq, dtype=jnp.float32) / half_freq)
    angles = t_index.astype(jnp.float32)[:, None] * freqs[None, :]
    freq_feat = jnp.concatenate([jnp.cos(angles), jnp.sin(angles)], axis=1).astype(jnp.bfloat16)
    t_hidden = jax.nn.silu(jnp.dot(freq_feat, t_w1, preferred_element_type=jnp.float32)).astype(jnp.bfloat16)
    t_embed = jnp.dot(t_hidden, t_w2, preferred_element_type=jnp.float32)
    onehot = (jnp.arange(class_table.shape[0], dtype=jnp.int32)[None, :] == labels[:, None]).astype(jnp.bfloat16)
    return t_embed + jnp.dot(onehot, class_table, preferred_element_type=jnp.float32)

def layer_norm(values):
    centre = lax.optimization_barrier(jnp.mean(values, axis=-1, keepdims=True))
    spread = lax.optimization_barrier(jnp.mean((values - centre) ** 2, axis=-1, keepdims=True))
    return (values - centre) * lax.rsqrt(spread + 1e-06)

def attend_image(operands):
    query, key, value, stale_key, stale_value = operands
    n_patch = N_ROW
    per_patch = TR * GC

    def to_patches(tensor):
        return tensor.reshape(n_patch, per_patch, HEADS, HD).astype(jnp.float32)
    query_p = to_patches(query)
    key_p = to_patches(key)
    value_p = to_patches(value)
    coarse_key = stale_key.reshape(LR * LC, HEADS, HD).astype(jnp.float32)
    coarse_value = stale_value.reshape(LR * LC, HEADS, HD).astype(jnp.float32)
    scale = 1.0 / math.sqrt(HD)
    fresh = jnp.einsum('pqhd,pkhd->phqk', query_p, key_p) * scale
    stale = jnp.einsum('pqhd,khd->phqk', query_p, coarse_key) * scale + math.log(4.0)
    key_patch = jnp.broadcast_to((jnp.arange(LR, dtype=jnp.int32) // (TR // 2))[:, None], (LR, LC)).reshape(LR * LC)
    own = key_patch[None, :] == jnp.arange(n_patch, dtype=jnp.int32)[:, None]
    stale = jnp.where(own[:, None, None, :], jnp.float32(-1e+30), stale)
    scores = jnp.concatenate([fresh, stale], axis=-1)
    weights = jax.nn.softmax(scores, axis=-1).astype(jnp.bfloat16).astype(jnp.float32)
    attended = jnp.einsum('phqk,pkhd->pqhd', weights[..., :per_patch], value_p)
    attended = attended + jnp.einsum('phqk,khd->pqhd', weights[..., per_patch:], coarse_value)
    return attended.reshape(GR, GC, HEADS * HD).astype(jnp.bfloat16)

def reference(x_lo, noise, t_index, labels, stale_kv, embed_w, t_w1, t_w2, class_table, ada_w, qkv_w, out_w, fc1_w, fc2_w):
    abar = noise_level(t_index)
    padded = jnp.pad(x_lo, ((0, 0), (1, 1), (1, 1), (0, 0)), mode='edge')
    upsampled = upsample_padded(padded)
    noisy = jnp.sqrt(abar)[:, None, None, None] * upsampled + jnp.sqrt(1.0 - abar)[:, None, None, None] * noise
    grouped = noisy.reshape(B, GR, GC, 4, C)
    count = 4.0 * GR * GC
    total = lax.optimization_barrier(jnp.sum(grouped, axis=(1, 2, 3)))
    squares = lax.optimization_barrier(jnp.sum(grouped * grouped, axis=(1, 2, 3)))
    centre = total / count
    spread = squares / count - centre * centre
    normed = ((grouped - centre[:, None, None, None, :]) * lax.rsqrt(spread + 1e-05)[:, None, None, None, :]).reshape(B, GR, GC, 4 * C)
    pos = position_table(jnp.arange(GR, dtype=jnp.float32), jnp.arange(GC, dtype=jnp.float32), D)
    tokens = (jnp.einsum('bijf,fd->bijd', normed, embed_w, precision=lax.Precision.HIGHEST) + pos[None]).astype(jnp.bfloat16)
    cond = condition(t_index, labels, t_w1, t_w2, class_table)
    cond_act = jax.nn.silu(cond).astype(jnp.bfloat16)
    modulation = jnp.dot(cond_act, ada_w, preferred_element_type=jnp.float32)
    shift1, scale1, gate1, shift2, scale2, gate2 = jnp.split(modulation, 6, axis=1)
    flat = tokens.astype(jnp.float32).reshape(B, GR * GC, D)
    normed1 = (layer_norm(flat) * (1.0 + scale1[:, None, :]) + shift1[:, None, :]).astype(jnp.bfloat16)
    qkv = jnp.dot(normed1.reshape(B * GR * GC, D), qkv_w.reshape(D, 3 * D), preferred_element_type=jnp.float32)
    qkv = qkv.astype(jnp.bfloat16).reshape(B, GR, GC, 3, HEADS, HD)
    stale = stale_kv.reshape(2, B, LR, LC, HEADS, HD)
    attended = lax.map(attend_image, (qkv[:, :, :, 0], qkv[:, :, :, 1], qkv[:, :, :, 2], stale[0], stale[1]))
    projected = jnp.dot(attended.reshape(B * GR * GC, D), out_w, preferred_element_type=jnp.float32).reshape(B, GR * GC, D)
    mid = (flat + gate1[:, None, :] * projected).astype(jnp.bfloat16)
    normed2 = (layer_norm(mid.astype(jnp.float32)) * (1.0 + scale2[:, None, :]) + shift2[:, None, :]).astype(jnp.bfloat16)
    hidden = jax.nn.gelu(jnp.dot(normed2.reshape(B * GR * GC, D), fc1_w, preferred_element_type=jnp.float32), approximate=True).astype(jnp.bfloat16)
    mlp_term = lax.dot_general(hidden, fc2_w, (((1,), (1,)), ((), ())), preferred_element_type=jnp.float32).reshape(B, GR * GC, D)
    tokens_out = (mid.astype(jnp.float32) + gate2[:, None, :] * mlp_term).astype(jnp.bfloat16)
    return tokens_out.reshape(B, GR, GC, D)
```

```python
import functools
import math

import jax
import jax.numpy as jnp
from jax import lax
from jax.experimental import pallas as pl
from jax.experimental.pallas import tpu as pltpu
from jax.sharding import PartitionSpec as P

HD = 72
TSTEPS = 1000
VMEM = 60 * 1024 * 1024


def rotation(count, step):
    return [(i, (i + step) % count) for i in range(count)]


def exchange(count, bit):
    return [(i, i ^ bit) for i in range(count)]


def noise_level(t_index):
    step_values = jnp.arange(TSTEPS, dtype=jnp.float32)
    betas = 0.0001 + (0.02 - 0.0001) * step_values / (TSTEPS - 1)
    kept = (jnp.arange(TSTEPS, dtype=jnp.int32)[None, :] <= t_index[:, None]).astype(jnp.float32)
    return jnp.exp(jnp.sum(kept * jnp.log(1.0 - betas)[None, :], axis=1))


def position_parts(row_pos, col_pos, width):
    quarter = width // 4
    omega = 1.0 / 10000.0 ** (jnp.arange(quarter, dtype=jnp.float32) / quarter)
    row_args = row_pos[:, None] * omega[None, :]
    col_args = col_pos[:, None] * omega[None, :]
    row_part = jnp.concatenate([jnp.sin(row_args), jnp.cos(row_args)], axis=1)
    col_part = jnp.concatenate([jnp.sin(col_args), jnp.cos(col_args)], axis=1)
    return jnp.pad(row_part, ((0, 0), (0, width // 2))), jnp.pad(
        col_part, ((0, 0), (width // 2, 0))
    )


def condition(t_index, labels, t_w1, t_w2, class_table):
    half_freq = t_w1.shape[0] // 2
    freqs = jnp.exp(-math.log(10000.0) * jnp.arange(half_freq, dtype=jnp.float32) / half_freq)
    angles = t_index.astype(jnp.float32)[:, None] * freqs[None, :]
    freq_feat = jnp.concatenate([jnp.cos(angles), jnp.sin(angles)], axis=1).astype(jnp.bfloat16)
    t_hidden = jax.nn.silu(jnp.dot(freq_feat, t_w1, preferred_element_type=jnp.float32)).astype(
        jnp.bfloat16
    )
    t_embed = jnp.dot(t_hidden, t_w2, preferred_element_type=jnp.float32)
    onehot = (jnp.arange(class_table.shape[0], dtype=jnp.int32)[None, :] == labels[:, None]).astype(
        jnp.bfloat16
    )
    return t_embed + jnp.dot(onehot, class_table, preferred_element_type=jnp.float32)


def split3(values):
    high = lax.reduce_precision(values, 8, 7)
    rest = values - high
    middle = lax.reduce_precision(rest, 8, 7)
    return jnp.stack([high, middle, rest - middle]).astype(jnp.bfloat16)


def layer_norm(values):
    centre = jnp.mean(values, axis=-1, keepdims=True)
    moved = values - centre
    spread = jnp.mean(moved * moved, axis=-1, keepdims=True)
    return moved * lax.rsqrt(spread + 1e-06)


def dot_t(left, right):
    return lax.dot_general(
        left, right, (((1,), (1,)), ((), ())), preferred_element_type=jnp.float32
    )


def qkv_kernel(nx_ref, embed_ref, row_ref, col_ref, mod_ref, w_ref, tok_ref, q_ref, k_ref, v_ref):
    parts, half, width = col_ref.shape
    tile_rows = row_ref.shape[0]
    raw = jnp.dot(
        nx_ref[0],
        embed_ref[...],
        precision=lax.Precision.HIGHEST,
        preferred_element_type=jnp.float32,
    ).reshape(parts, tile_rows, half, width)
    pos = row_ref[...][None, :, None, :] + col_ref[...][:, None, :, :]
    tokens = (raw + pos).reshape(parts * tile_rows * half, width).astype(jnp.bfloat16)
    tok_ref[0] = tokens
    normed = (
        layer_norm(tokens.astype(jnp.float32)) * (1.0 + mod_ref[0, 1:2]) + mod_ref[0, 0:1]
    ).astype(jnp.bfloat16)
    q_ref[0] = dot_t(normed, w_ref[0]).astype(jnp.bfloat16)
    k_ref[0] = dot_t(normed, w_ref[1]).astype(jnp.bfloat16)
    v_ref[0] = dot_t(normed, w_ref[2]).astype(jnp.bfloat16)


def attend_kernel(pieces, q_ref, k_ref, v_ref, *refs):
    stale = refs[:pieces]
    out_ref, k_all, v_all, acc = refs[pieces:]
    tokens, local = q_ref.shape[1:]
    k_all[:tokens] = k_ref[0]
    v_all[:tokens] = v_ref[0]
    at = tokens
    for ref in stale:
        count = ref.shape[2]
        k_all[at : at + count] = ref[0, 0]
        v_all[at : at + count] = ref[1, 0]
        at += count
    scale = math.log2(math.e) / math.sqrt(HD)
    bias = jnp.where(lax.broadcasted_iota(jnp.int32, (1, at), 1) < tokens, 0.0, 2.0)
    for head in range(local // HD):
        low, high = head * HD, (head + 1) * HD
        start = low // 128 * 128
        stop = min(-(-high // 128) * 128, local)
        lane = lax.broadcasted_iota(jnp.int32, (1, stop - start), 1) + start
        mine = (lane >= low) & (lane < high)
        query = q_ref[0, :, start:stop]
        query = jnp.where(mine, query, jnp.zeros_like(query))
        scores = dot_t(query, k_all[:, start:stop]) * scale + bias
        top = jnp.max(scores, axis=-1, keepdims=True)
        weights = jnp.exp2(scores - top)
        mass = jnp.sum(weights, axis=-1, keepdims=True)
        part = jnp.dot(
            weights.astype(jnp.bfloat16), v_all[:, start:stop], preferred_element_type=jnp.float32
        )
        part = part / mass
        if low == start:
            acc[:, start:stop] = part
        else:
            acc[:, start:stop] = jnp.where(mine, part, acc[:, start:stop])
    out_ref[0] = acc[...].astype(jnp.bfloat16)


def gelu(values):
    inner = math.sqrt(2.0 / math.pi) * (values + 0.044715 * values * values * values)
    return 0.5 * values * (1.0 + jnp.tanh(inner))


def mlp_kernel(heads, others, *refs):
    att = refs[:heads]
    refs = refs[heads:]
    tok_ref, mod_ref = refs[:2]
    out_w = refs[2 : 2 + heads]
    refs = refs[2 + heads :]
    weights = refs[: 2 + 4 * others]
    keep_ref, send_ref, wo, w1, w2, sems = refs[2 + 4 * others :]
    step = pl.program_id(0)
    width = tok_ref.shape[-1]
    parity = lax.rem(lax.axis_index("row"), 2)
    rows = width // 2
    mine = pl.ds(pl.multiple_of(parity * rows, rows), rows)
    theirs = pl.ds(pl.multiple_of((1 - parity) * rows, rows), rows)
    copies_o = [
        pltpu.make_async_copy(out_w[j], wo.at[j], sems.at[j]) for j in range(heads)
    ]
    pairs1 = [(weights[0], w1.at[0])]
    pairs2 = [(weights[1], w2.at[0])]
    for s in range(others):
        base = 2 + 4 * s
        pairs1 += [(weights[base], w1.at[1 + s, mine]), (weights[base + 1], w1.at[1 + s, theirs])]
        pairs2 += [
            (weights[base + 2], w2.at[1 + s, mine]),
            (weights[base + 3], w2.at[1 + s, theirs]),
        ]
    copies_1 = [
        pltpu.make_async_copy(a, b, sems.at[heads + i]) for i, (a, b) in enumerate(pairs1)
    ]
    copies_2 = [
        pltpu.make_async_copy(a, b, sems.at[heads + len(pairs1) + i])
        for i, (a, b) in enumerate(pairs2)
    ]

    @pl.when(step == 0)
    def _():
        for copy in copies_o + copies_1 + copies_2:
            copy.start()
        for copy in copies_o:
            copy.wait()

    block = att[0].shape[2]
    proj = None
    for j in range(heads):
        if j == 0:
            values = att[0][0].reshape(heads * block, -1)
        else:
            values = jnp.concatenate([att[j][0, (m - j) % heads] for m in range(heads)], axis=0)
        term = jnp.dot(values, wo[j], preferred_element_type=jnp.float32)
        proj = term if proj is None else proj + term
    mid = (tok_ref[0].astype(jnp.float32) + mod_ref[0, 2:3] * proj).astype(jnp.bfloat16)
    mid = mid.astype(jnp.float32)
    normed = (layer_norm(mid) * (1.0 + mod_ref[0, 4:5]) + mod_ref[0, 3:4]).astype(jnp.bfloat16)

    @pl.when(step == 0)
    def _():
        for copy in copies_1:
            copy.wait()

    hidden = [
        gelu(jnp.dot(normed, w1[c], preferred_element_type=jnp.float32)).astype(jnp.bfloat16)
        for c in range(1 + others)
    ]

    @pl.when(step == 0)
    def _():
        for copy in copies_2:
            copy.wait()

    out = None
    for c in range(1 + others):
        term = dot_t(hidden[c], w2[c])
        out = term if out is None else out + term
    keep_ref[0] = mid[:block] + mod_ref[0, 5:6] * out[:block]
    for j in range(1, heads):
        send_ref[j - 1, 0] = out[j * block : (j + 1) * block].astype(jnp.bfloat16)


def body(
    x_lo,
    noise,
    t_index,
    labels,
    stale_kv,
    embed_w,
    t_w1,
    t_w2,
    class_table,
    ada_w,
    qkv_w,
    out_w,
    fc1_w,
    fc2_w,
):
    row = lax.axis_index("row")
    rows = lax.axis_size("row")
    head = lax.axis_index("head")
    heads = lax.axis_size("head")
    cols = lax.axis_size("col")
    batch, tile_rows, full_cols, features = noise.shape
    channels = x_lo.shape[3]
    width = embed_w.shape[1]
    local = qkv_w.shape[2]
    half = full_cols // heads
    block = tile_rows * half
    tokens_n = tile_rows * full_cols
    pair = exchange(rows, 1)

    wide = jnp.concatenate(
        [x_lo] + [lax.ppermute(x_lo, "head", rotation(heads, -j)) for j in range(1, heads)], axis=2
    )
    forward = [(i, i + 1) for i in range(rows - 1)]
    backward = [(i + 1, i) for i in range(rows - 1)]
    above = lax.ppermute(wide[:, -1:], "row", forward)
    below = lax.ppermute(wide[:, :1], "row", backward)

    cond_act = jax.nn.silu(condition(t_index, labels, t_w1, t_w2, class_table)).astype(jnp.bfloat16)
    mod = jnp.dot(cond_act, ada_w, preferred_element_type=jnp.float32)

    above = jnp.where(row == 0, wide[:, :1], above)
    below = jnp.where(row == rows - 1, wide[:, -1:], below)
    padded = jnp.concatenate([above, wide, below], axis=1)
    middle = padded[:, 1:-1]
    col_at = (jnp.arange(full_cols, dtype=jnp.int32) + head * half) % full_cols

    def widen(vertical):
        left = jnp.roll(vertical, 1, axis=2)
        left = jnp.where((col_at == 0)[None, None, :, None], vertical, left)
        right = jnp.roll(vertical, -1, axis=2)
        right = jnp.where((col_at == full_cols - 1)[None, None, :, None], vertical, right)
        return [0.75 * vertical + 0.25 * left, 0.75 * vertical + 0.25 * right]

    upsampled = jnp.concatenate(
        widen(0.75 * middle + 0.25 * padded[:, :-2]) + widen(0.75 * middle + 0.25 * padded[:, 2:]),
        axis=3,
    )
    rolled = lax.dynamic_slice_in_dim(
        jnp.concatenate([noise, noise], axis=2), head * half, full_cols, 2
    )
    abar = noise_level(t_index)
    noisy = (
        jnp.sqrt(abar)[:, None, None, None] * upsampled
        + jnp.sqrt(1.0 - abar)[:, None, None, None] * rolled
    )
    sums = jnp.stack([jnp.sum(noisy, axis=(1, 2)), jnp.sum(noisy * noisy, axis=(1, 2))])
    sums = jnp.sum(sums.reshape(2, batch, features // channels, channels), axis=2)

    bit = 1
    while bit < rows:
        triple = split3(sums).reshape(1, -1)
        triple = jnp.pad(triple, ((0, 0), (0, mod.shape[1] - triple.shape[1])))
        got = lax.ppermute(
            jnp.concatenate([mod.astype(jnp.bfloat16), triple], axis=0), "row", exchange(rows, bit)
        )
        got = got.astype(jnp.float32)
        mod = mod + got[:batch]
        sums = sums + jnp.sum(
            got[batch, : 3 * sums.size].reshape((3,) + sums.shape), axis=0
        )
        bit *= 2

    count = float(4 * tile_rows * rows * full_cols)
    centre = sums[0] / count
    spread = sums[1] / count - centre * centre
    repeat = features // channels
    normed = (noisy - jnp.tile(centre, (1, repeat))[:, None, None, :]) * jnp.tile(
        lax.rsqrt(spread + 1e-05), (1, repeat)
    )[:, None, None, :]
    normed = (
        normed.reshape(batch, tile_rows, heads, half, features)
        .transpose(0, 2, 1, 3, 4)
        .reshape(batch, tokens_n, features)
    )
    mod = mod.reshape(batch, 6, width)

    row_at = (row * tile_rows + jnp.arange(tile_rows, dtype=jnp.int32)).astype(jnp.float32)
    row_part, col_part = position_parts(row_at, col_at.astype(jnp.float32), width)
    params = pltpu.CompilerParams(vmem_limit_bytes=VMEM)
    whole = lambda shape: pl.BlockSpec(shape, lambda b: (0,) * len(shape))
    image = lambda *shape: pl.BlockSpec((1,) + shape, lambda b: (b,) + (0,) * len(shape))
    tokens, query, key, value = pl.pallas_call(
        qkv_kernel,
        grid=(batch,),
        in_specs=[
            image(tokens_n, features),
            whole((features, width)),
            whole((tile_rows, width)),
            whole((heads, half, width)),
            image(6, width),
            whole((3, local, width)),
        ],
        out_specs=[image(tokens_n, width)] + [image(tokens_n, local)] * 3,
        out_shape=[jax.ShapeDtypeStruct((batch, tokens_n, width), jnp.bfloat16)]
        + [jax.ShapeDtypeStruct((batch, tokens_n, local), jnp.bfloat16)] * 3,
        compiler_params=params,
        name="embed_qkv",
    )(
        normed,
        embed_w,
        row_part,
        col_part.reshape(heads, half, width),
        mod,
        qkv_w.transpose(1, 2, 0),
    )

    stale = stale_kv.reshape(2, batch, -1, local)
    mine = [stale]
    for chip in range(1, rows // 2):
        mine.append(lax.ppermute(stale, "row", rotation(rows, 2 * chip)))
    pieces = mine[1:] + [lax.ppermute(piece, "row", pair) for piece in mine]
    per_piece = stale.shape[2]
    keys_n = tokens_n + len(pieces) * per_piece
    attended = pl.pallas_call(
        functools.partial(attend_kernel, len(pieces)),
        grid=(batch,),
        in_specs=[image(tokens_n, local)] * 3
        + [pl.BlockSpec((2, 1, per_piece, local), lambda b: (0, b, 0, 0))] * len(pieces),
        out_specs=image(tokens_n, local),
        out_shape=jax.ShapeDtypeStruct((batch, tokens_n, local), jnp.bfloat16),
        scratch_shapes=[
            pltpu.VMEM((keys_n, local), jnp.bfloat16),
            pltpu.VMEM((keys_n, local), jnp.bfloat16),
            pltpu.VMEM((tokens_n, local), jnp.float32),
        ],
        compiler_params=params,
        name="attend",
    )(query, key, value, *pieces)

    out_ws = [out_w] + [lax.ppermute(out_w, "head", rotation(heads, -j)) for j in range(1, heads)]
    parity = row % 2
    weights = [fc1_w, fc2_w]
    for s in range(1, cols):
        for matrix in (fc1_w, fc2_w):
            part = lax.dynamic_slice_in_dim(matrix, parity * (width // 2), width // 2, 0)
            part = lax.ppermute(part, "col", rotation(cols, s))
            weights += [part, lax.ppermute(part, "row", pair)]

    attended = attended.reshape(batch, heads, block, local)
    atts = [attended] + [
        lax.ppermute(attended, "head", rotation(heads, -j)) for j in range(1, heads)
    ]
    anywhere = pl.BlockSpec(memory_space=pl.ANY)
    hidden_n = fc1_w.shape[1]
    keep, send = pl.pallas_call(
        functools.partial(mlp_kernel, heads, cols - 1),
        grid=(batch,),
        in_specs=[image(heads, block, local)] * heads
        + [image(tokens_n, width), image(6, width)]
        + [anywhere] * (heads + len(weights)),
        out_specs=[
            image(block, width),
            pl.BlockSpec((heads - 1, 1, block, width), lambda b: (0, b, 0, 0)),
        ],
        out_shape=[
            jax.ShapeDtypeStruct((batch, block, width), jnp.float32),
            jax.ShapeDtypeStruct((heads - 1, batch, block, width), jnp.bfloat16),
        ],
        scratch_shapes=[
            pltpu.VMEM((heads, local, width), jnp.bfloat16),
            pltpu.VMEM((cols, width, hidden_n), jnp.bfloat16),
            pltpu.VMEM((cols, width, hidden_n), jnp.bfloat16),
            pltpu.SemaphoreType.DMA((heads + len(weights),)),
        ],
        compiler_params=params,
        name="project_mlp",
    )(*atts, tokens, mod, *out_ws, *weights)
    total = sum(
        lax.ppermute(send[j - 1], "head", rotation(heads, j)).astype(jnp.float32)
        for j in range(1, heads)
    )
    result = (keep + mod[:, 5][:, None, :] * total).astype(jnp.bfloat16)
    return result.reshape(batch, tile_rows, half, width)


def solution(mesh):
    placed = (
        P("col", "row", "head", None),
        P("col", "row", None, None),
        P("col"),
        P("col"),
        P(None, "col", "row", None, "head"),
        P(),
        P(),
        P(None, "row"),
        P(None, "row"),
        P("row", None),
        P(None, None, "head"),
        P("head", None),
        P(None, ("col", "head")),
        P(None, ("col", "head")),
    )
    return jax.shard_map(
        body, mesh=mesh, in_specs=placed, out_specs=P("col", "row", "head", None), check_vma=False
    )
```
